16 devices in a mesh: sp: 16 (over z, y, x, core).
Axes of the slice: x: 2, y: 2, z: 2, core: 2. Of those that a mesh axis runs over, the one named last changes fastest.
Arguments:
- x: bfloat16 [32, 512, 4096], P(None, 'sp')
- dy: bfloat16 [32, 512, 4096], P(None, 'sp')
- prefix_len: int32 [32], replicated
- w_norm: bfloat16 [4096], replicated
- w_q: bfloat16 [4096, 4096], replicated
- w_k: bfloat16 [4096, 128], replicated
- w_v: bfloat16 [4096, 128], replicated
- w_o: bfloat16 [4096, 4096], replicated
Outputs:
- output 1: bfloat16 [32, 512, 4096], P(None, 'sp')
- output 2: bfloat16 [32, 512, 4096], P(None, 'sp')
- output 3: float32 [4096, 4096], replicated
- output 4: float32 [4096, 128], replicated
- output 5: float32 [4096, 128], replicated
- output 6: float32 [4096, 4096], replicated
- output 7: float32 [4096], replicated
All inputs are finite; a program needn't handle non-finite values.
Results may differ from the reference program's by a relative error of at most 0.0128496.
Values are sent between devices in bfloat16 or wider.
A program may use at most 1 GiB of HBM per device.

```python
import math
import functools
import jax
import jax.numpy as jnp
from jax import lax

BATCH = 32
SEQ_LEN = 512
D_MODEL = 4096
HEADS = 32
HEAD_DIM = 128

ROPE_THETA = 10000.0
NORM_EPS = 1e-6
MASK_FILL = -1e30
ROW_BLOCK = math.gcd(SEQ_LEN, 256)


def setup_inputs(seed: int = 0) -> dict:
    keys = jax.random.split(jax.random.key(seed), 9)
    q_width = HEADS * HEAD_DIM
    x = jax.random.normal(keys[0], (BATCH, SEQ_LEN, D_MODEL), jnp.float32)
    dy = jax.random.normal(keys[1], (BATCH, SEQ_LEN, D_MODEL), jnp.float32)
    prefix_low = SEQ_LEN // 8
    prefix_high = 7 * SEQ_LEN // 8
    drawn_lens = jax.random.randint(keys[2], (BATCH,), prefix_low, prefix_high + 1, dtype=jnp.int32)
    drawn_lens = drawn_lens.at[0].set(prefix_low).at[1].set(prefix_high)
    prefix_len = jax.random.permutation(keys[3], drawn_lens)
    w_norm = 0.5 * jax.random.normal(keys[4], (D_MODEL,), jnp.float32)
    w_q = 1.2 * D_MODEL ** -0.5 * jax.random.normal(keys[5], (D_MODEL, q_width), jnp.float32)
    w_k = 1.2 * D_MODEL ** -0.5 * jax.random.normal(keys[6], (D_MODEL, HEAD_DIM), jnp.float32)
    w_v = D_MODEL ** -0.5 * jax.random.normal(keys[7], (D_MODEL, HEAD_DIM), jnp.float32)
    w_o = 2.0 * q_width ** -0.5 * jax.random.normal(keys[8], (q_width, D_MODEL), jnp.float32)
    return {'x': x.astype(jnp.bfloat16), 'dy': dy.astype(jnp.bfloat16), 'prefix_len': prefix_len, 'w_norm': w_norm.astype(jnp.bfloat16), 'w_q': w_q.astype(jnp.bfloat16), 'w_k': w_k.astype(jnp.bfloat16), 'w_v': w_v.astype(jnp.bfloat16), 'w_o': w_o.astype(jnp.bfloat16)}


def to_bf16_grid(values):
    return values.astype(jnp.bfloat16).astype(jnp.float32)


def rope_tables(positions):
    half = HEAD_DIM // 2
    frequencies = ROPE_THETA ** (-2.0 * jnp.arange(half, dtype=jnp.float32) / HEAD_DIM)
    angles = positions.astype(jnp.float32)[:, None] * frequencies[None, :]
    return jnp.cos(angles), jnp.sin(angles)


def apply_rope(vectors, cos_tab, sin_tab):
    half = vectors.shape[-1] // 2
    first = vectors[..., :half]
    second = vectors[..., half:]
    return jnp.concatenate([first * cos_tab - second * sin_tab, second * cos_tab + first * sin_tab], axis=-1)


def attend_sequence(item):
    q_seq, k_seq, v_seq, prefix = item
    key_pos = jnp.arange(SEQ_LEN)

    def one_block(block_item):
        q_rows, start = block_item
        row_pos = start + jnp.arange(ROW_BLOCK)
        visible = (key_pos[None, :] < prefix) | (key_pos[None, :] <= row_pos[:, None])
        scores = jnp.einsum('qhe,ke->hqk', q_rows, k_seq)
        scores = jnp.where(visible[None], scores, MASK_FILL)
        attn_probs = to_bf16_grid(jax.nn.softmax(scores, axis=-1))
        return to_bf16_grid(jnp.einsum('hqk,ke->qhe', attn_probs, v_seq))

    blocks = q_seq.reshape(SEQ_LEN // ROW_BLOCK, ROW_BLOCK, HEADS, HEAD_DIM)
    starts = jnp.arange(SEQ_LEN // ROW_BLOCK) * ROW_BLOCK
    attn_out = lax.map(jax.checkpoint(one_block), (blocks, starts))
    return attn_out.reshape(SEQ_LEN, HEADS, HEAD_DIM)


def block_forward(x, gain, w_q, w_k, w_v, w_o, prefix_len):
    x_f32 = x.astype(jnp.float32)
    inv_rms = lax.rsqrt(jnp.mean(x_f32 * x_f32, axis=-1, keepdims=True) + NORM_EPS)
    normed = to_bf16_grid(x_f32 * inv_rms * (1.0 + gain))
    cos_tab, sin_tab = rope_tables(jnp.arange(SEQ_LEN))
    q_proj = jnp.einsum('bsd,de->bse', normed, w_q).reshape(BATCH, SEQ_LEN, HEADS, HEAD_DIM)
    queries = to_bf16_grid(apply_rope(q_proj, cos_tab[:, None, :], sin_tab[:, None, :]) * HEAD_DIM ** -0.5)
    keys = to_bf16_grid(apply_rope(jnp.einsum('bsd,de->bse', normed, w_k), cos_tab, sin_tab))
    values = to_bf16_grid(jnp.einsum('bsd,de->bse', normed, w_v))
    attn_out = lax.map(attend_sequence, (queries, keys, values, prefix_len))
    mixed = jnp.einsum('bse,ed->bsd', attn_out.reshape(BATCH, SEQ_LEN, HEADS * HEAD_DIM), w_o)
    return (x_f32 + mixed).astype(jnp.bfloat16)


def reference(x, dy, prefix_len, w_norm, w_q, w_k, w_v, w_o):
    forward = functools.partial(block_forward, prefix_len=prefix_len)
    y_out, pull_back = jax.vjp(forward, x, w_norm.astype(jnp.float32), w_q.astype(jnp.float32), w_k.astype(jnp.float32), w_v.astype(jnp.float32), w_o.astype(jnp.float32))
    dx_out, d_gain, d_wq, d_wk, d_wv, d_wo = pull_back(dy)
    return y_out, dx_out, d_wq, d_wk, d_wv, d_wo, d_gain
```

```python
import functools
import jax
import jax.numpy as jnp
from jax import lax
from jax.experimental import pallas as pl
from jax.experimental.pallas import tpu as pltpu
from jax.sharding import PartitionSpec as P

ROPE_THETA = 10000.0
NORM_EPS = 1e-6
MASK_FILL = -1e30
GROUP_HEADS = 8


def rope_tables(positions, head_dim):
    half = head_dim // 2
    frequencies = ROPE_THETA ** (-2.0 * jnp.arange(half, dtype=jnp.float32) / head_dim)
    angles = positions.astype(jnp.float32)[:, None] * frequencies[None, :]
    return jnp.cos(angles), jnp.sin(angles)


def apply_rope(vectors, cos_tab, sin_tab):
    half = vectors.shape[-1] // 2
    first = vectors[..., :half]
    second = vectors[..., half:]
    return jnp.concatenate([first * cos_tab - second * sin_tab, second * cos_tab + first * sin_tab], axis=-1)


def rms_norm(x_f32, gain):
    inv_rms = lax.rsqrt(jnp.mean(x_f32 * x_f32, axis=-1, keepdims=True) + NORM_EPS)
    return x_f32 * inv_rms * (1.0 + gain)


def attention_kernel(heads, scale, prefix_ref, base_ref, q_ref, do_ref, kv_ref, cos_ref, sin_ref, cost_ref, sint_ref,
                     o_ref, dq_ref, dk_ref, dv_ref, cap_ref):
    b = pl.program_id(0)
    tokens = q_ref.shape[1]
    e = kv_ref.shape[2] // 2
    n_keys = kv_ref.shape[1]
    rows = GROUP_HEADS * tokens
    prefix = prefix_ref[b]
    key_pos = lax.broadcasted_iota(jnp.int32, (n_keys, rows), 0)
    token = lax.rem(lax.broadcasted_iota(jnp.int32, (n_keys, rows), 1), tokens) + base_ref[0]
    cap_ref[...] = jnp.where((key_pos < prefix) | (key_pos <= token), jnp.inf, MASK_FILL)

    k = kv_ref[0, :, :e]
    v = kv_ref[0, :, e:]
    k_t = k.T
    v_t = v.T
    cos = cos_ref[...]
    sin = sin_ref[...]
    nt = (((1,), (1,)), ((), ()))
    nn = (((1,), (0,)), ((), ()))
    f32 = jnp.float32
    dk = None
    for g in range(heads // GROUP_HEADS):
        cols = [slice((g * GROUP_HEADS + i) * e, (g * GROUP_HEADS + i + 1) * e) for i in range(GROUP_HEADS)]
        q_raw = jnp.concatenate([q_ref[0, :, c] for c in cols], axis=0)
        q = ((q_raw * cos + pltpu.roll(q_raw, e // 2, 1) * sin) * scale).astype(jnp.bfloat16)
        do = jnp.concatenate([do_ref[0, :, c] for c in cols], axis=0)
        s = jnp.minimum(lax.dot_general(k, q, nt, preferred_element_type=f32), cap_ref[...])
        p = jnp.exp(s - jnp.max(s, axis=0, keepdims=True))
        p = p * (1.0 / jnp.sum(p, axis=0, keepdims=True))
        p_b = p.astype(jnp.bfloat16)
        dp = lax.dot_general(v, do, nt, preferred_element_type=f32).astype(jnp.bfloat16).astype(f32)
        delta = jnp.sum(dp * p, axis=0, keepdims=True)
        ds = (p * (dp - delta)).astype(jnp.bfloat16)
        o_t = lax.dot_general(v_t, p_b, nn, preferred_element_type=f32)
        dq_t = lax.dot_general(k_t, ds, nn, preferred_element_type=f32).astype(jnp.bfloat16).astype(f32) * scale
        dq_t = dq_t * cost_ref[...] - jnp.concatenate([dq_t[e // 2:], dq_t[:e // 2]], axis=0) * sint_ref[...]
        o = o_t.T.astype(jnp.bfloat16)
        dq = dq_t.T.astype(jnp.bfloat16)
        for i, c in enumerate(cols):
            o_ref[0, :, c] = o[i * tokens:(i + 1) * tokens]
            dq_ref[0, :, c] = dq[i * tokens:(i + 1) * tokens]
        dk_g = lax.dot_general(ds, q, nn, preferred_element_type=f32)
        dv_g = lax.dot_general(p_b, do, nn, preferred_element_type=f32)
        if g == 0:
            dk_ref[0], dv_ref[0] = dk_g, dv_g
        else:
            dk_ref[0] += dk_g
            dv_ref[0] += dv_g


def attention(q_proj, do, kv, prefix_len, base, cos_tab, sin_tab, scale):
    batch, tokens, width = q_proj.shape
    e = kv.shape[2] // 2
    n_keys = kv.shape[1]
    heads = width // e
    cos_one = jnp.concatenate([cos_tab, cos_tab], axis=1)
    sin_one = jnp.concatenate([-sin_tab, sin_tab], axis=1)
    cos_full = jnp.tile(cos_one, (GROUP_HEADS, 1))
    sin_full = jnp.tile(sin_one, (GROUP_HEADS, 1))
    rows = GROUP_HEADS * tokens
    tok_spec = pl.BlockSpec((1, tokens, width), lambda b, *_: (b, 0, 0))
    kv_spec = pl.BlockSpec((1, n_keys, 2 * e), lambda b, *_: (b, 0, 0))
    dk_spec = pl.BlockSpec((1, n_keys, e), lambda b, *_: (b, 0, 0))
    tab_spec = pl.BlockSpec((rows, e), lambda b, *_: (0, 0))
    tab_t_spec = pl.BlockSpec((e, rows), lambda b, *_: (0, 0))
    flops = 6 * 2 * batch * heads * tokens * n_keys * e
    return pl.pallas_call(
        functools.partial(attention_kernel, heads, scale),
        grid_spec=pltpu.PrefetchScalarGridSpec(
            num_scalar_prefetch=2,
            grid=(batch,),
            in_specs=[tok_spec, tok_spec, kv_spec, tab_spec, tab_spec, tab_t_spec, tab_t_spec],
            out_specs=[tok_spec, tok_spec, dk_spec, dk_spec],
            scratch_shapes=[pltpu.VMEM((n_keys, rows), jnp.float32)],
        ),
        out_shape=[
            jax.ShapeDtypeStruct((batch, tokens, width), jnp.bfloat16),
            jax.ShapeDtypeStruct((batch, tokens, width), jnp.bfloat16),
            jax.ShapeDtypeStruct((batch, n_keys, e), jnp.float32),
            jax.ShapeDtypeStruct((batch, n_keys, e), jnp.float32),
        ],
        cost_estimate=pl.CostEstimate(flops=2 * flops, bytes_accessed=q_proj.size * 10 + kv.size * 10, transcendentals=batch * heads * tokens * n_keys),
        compiler_params=pltpu.CompilerParams(dimension_semantics=("arbitrary",), vmem_limit_bytes=40 * 1024 * 1024),
        name="attention",
    )(prefix_len, base, q_proj, do, kv, cos_full, sin_full, cos_full.T, sin_full.T)


def solution(mesh):
    groups = mesh.shape['sp']
    seq_spec = P(None, 'sp', None)
    whole = P()

    def local_block(x, dy, prefix_len, w_norm, w_q, w_k, w_v, w_o):
        batch, tokens, d_model = x.shape
        head_dim = w_k.shape[1]
        scale = head_dim ** -0.5
        my_index = lax.axis_index('sp')
        f32 = jnp.float32

        x_f32 = x.astype(f32)
        normed_f32, norm_pull = jax.vjp(rms_norm, x_f32, w_norm.astype(f32))
        normed = normed_f32.astype(jnp.bfloat16)
        base = my_index * tokens
        cos_tab, sin_tab = rope_tables(base + jnp.arange(tokens), head_dim)
        k_own = apply_rope(jnp.einsum('bsd,de->bse', normed, w_k, preferred_element_type=f32), cos_tab, sin_tab).astype(jnp.bfloat16)
        v_own = jnp.einsum('bsd,de->bse', normed, w_v, preferred_element_type=f32).astype(jnp.bfloat16)
        kv = lax.all_gather(jnp.concatenate([k_own, v_own], axis=-1), 'sp', axis=1, tiled=True)
        q_proj = jnp.einsum('bsd,de->bse', normed, w_q, preferred_element_type=f32)
        do = jnp.einsum('bsd,ed->bse', dy, w_o, preferred_element_type=f32).astype(jnp.bfloat16)
        o, dq_proj, dk_part, dv_part = attention(q_proj, do, kv, prefix_len, base.reshape(1), cos_tab, sin_tab, scale)

        dkv_own = lax.psum_scatter(jnp.stack([dk_part, dv_part]), 'sp', scatter_dimension=2, tiled=True)
        dk_own = dkv_own[0].astype(jnp.bfloat16)
        dv_own = dkv_own[1].astype(jnp.bfloat16)
        d_wo = jnp.einsum('bse,bsd->ed', o, dy, preferred_element_type=f32)
        d_wq = jnp.einsum('bsd,bse->de', normed, dq_proj, preferred_element_type=f32)
        mixed = jnp.einsum('bse,ed->bsd', o, w_o, preferred_element_type=f32)
        y_out = (x_f32 + mixed).astype(jnp.bfloat16)

        dk_proj = apply_rope(dk_own.astype(f32), cos_tab, -sin_tab).astype(jnp.bfloat16)
        d_wk = jnp.einsum('bsd,bse->de', normed, dk_proj, preferred_element_type=f32)
        d_wv = jnp.einsum('bsd,bse->de', normed, dv_own, preferred_element_type=f32)
        d_normed = (jnp.einsum('bse,de->bsd', dq_proj, w_q, preferred_element_type=f32)
                    + jnp.einsum('bse,de->bsd', dk_proj, w_k, preferred_element_type=f32)
                    + jnp.einsum('bse,de->bsd', dv_own, w_v, preferred_element_type=f32))
        dx_norm, d_gain = norm_pull(d_normed.astype(jnp.bfloat16).astype(f32))
        dx_out = (dy.astype(f32) + dx_norm).astype(jnp.bfloat16)
        d_wo = lax.psum(d_wo, 'sp')
        d_wq = lax.psum(d_wq, 'sp')
        d_wk, d_wv, d_gain = lax.psum((d_wk, d_wv, d_gain), 'sp')
        return y_out, dx_out, d_wq, d_wk, d_wv, d_wo, d_gain

    return jax.shard_map(local_block, mesh=mesh, in_specs=(seq_spec, seq_spec, whole, whole, whole, whole, whole, whole), out_specs=(seq_spec, seq_spec, whole, whole, whole, whole, whole), check_vma=False)
```

```python
import functools
import jax
import jax.numpy as jnp
from jax import lax
from jax.experimental import pallas as pl
from jax.experimental.pallas import tpu as pltpu
from jax.sharding import PartitionSpec as P

ROPE_THETA = 10000.0
NORM_EPS = 1e-6
MASK_FILL = -1e30
GROUP_HEADS = 8
KERNEL_Q_HEADS = 31
TILE = 128
SUB_TILES = 8
AG_DEPTH = 5
SIB_DEPTH = 3
A_DEPTH = 3
KV_DEPTH = 5
ROTATIONS = 3
SHIFT = 30
STAGES = 12
ST_CORE, ST_RS2, ST_RS3, ST_AG3, ST_AG2, ST_AG1, ST_SIB, ST_A, ST_K0, ST_K1, ST_K2, ST_K3 = range(STAGES)
JOB_COLS = 256
JOB_DEPTH = 512
JOB_FIRST = 10
GAIN_FIRST = 42
MESH_ID = pl.DeviceIdType.MESH
NT = (((1,), (1,)), ((), ()))


def rope_tables(positions, head_dim):
    half = head_dim // 2
    frequencies = ROPE_THETA ** (-2.0 * jnp.arange(half, dtype=jnp.float32) / head_dim)
    angles = positions.astype(jnp.float32)[:, None] * frequencies[None, :]
    return jnp.cos(angles), jnp.sin(angles)


def apply_rope(vectors, cos_tab, sin_tab):
    half = vectors.shape[-1] // 2
    first = vectors[..., :half]
    second = vectors[..., half:]
    return jnp.concatenate([first * cos_tab - second * sin_tab, second * cos_tab + first * sin_tab], axis=-1)


def attention_kernel(heads, scale, prefix_ref, base_ref, q_ref, do_ref, kv_ref, cos_ref, sin_ref, cost_ref, sint_ref,
                     o_ref, dq_ref, dkv_ref, cap_ref):
    b = pl.program_id(0)
    tokens = q_ref.shape[1]
    e = kv_ref.shape[2] // 2
    n_keys = kv_ref.shape[1]
    rows = GROUP_HEADS * tokens
    prefix = prefix_ref[b]
    key_pos = lax.broadcasted_iota(jnp.int32, (n_keys, rows), 0)
    token = lax.rem(lax.broadcasted_iota(jnp.int32, (n_keys, rows), 1), tokens) + base_ref[0]
    cap_ref[...] = jnp.where((key_pos < prefix) | (key_pos <= token), jnp.inf, MASK_FILL)

    k = kv_ref[0, :, :e]
    v = kv_ref[0, :, e:]
    k_t = k.T
    v_t = v.T
    cos = cos_ref[...]
    sin = sin_ref[...]
    nt = (((1,), (1,)), ((), ()))
    nn = (((1,), (0,)), ((), ()))
    f32 = jnp.float32
    dk = None
    for g in range(heads // GROUP_HEADS):
        cols = [slice((g * GROUP_HEADS + i) * e, (g * GROUP_HEADS + i + 1) * e) for i in range(GROUP_HEADS)]
        q_raw = jnp.concatenate([q_ref[0, :, c] for c in cols], axis=0)
        q = ((q_raw * cos + pltpu.roll(q_raw, e // 2, 1) * sin) * scale).astype(jnp.bfloat16)
        do = jnp.concatenate([do_ref[0, :, c] for c in cols], axis=0)
        s = jnp.minimum(lax.dot_general(k, q, nt, preferred_element_type=f32), cap_ref[...])
        p = jnp.exp(s - jnp.max(s, axis=0, keepdims=True))
        p = p * (1.0 / jnp.sum(p, axis=0, keepdims=True))
        p_b = p.astype(jnp.bfloat16)
        dp = lax.dot_general(v, do, nt, preferred_element_type=f32).astype(jnp.bfloat16).astype(f32)
        delta = jnp.sum(dp * p, axis=0, keepdims=True)
        ds = (p * (dp - delta)).astype(jnp.bfloat16)
        o_t = lax.dot_general(v_t, p_b, nn, preferred_element_type=f32)
        dq_t = lax.dot_general(k_t, ds, nn, preferred_element_type=f32).astype(jnp.bfloat16).astype(f32) * scale
        dq_t = dq_t * cost_ref[...] - jnp.concatenate([dq_t[e // 2:], dq_t[:e // 2]], axis=0) * sint_ref[...]
        o = o_t.T.astype(jnp.bfloat16)
        dq = dq_t.T.astype(jnp.bfloat16)
        for i, c in enumerate(cols):
            o_ref[0, :, c] = o[i * tokens:(i + 1) * tokens]
            dq_ref[0, :, c] = dq[i * tokens:(i + 1) * tokens]
        dk_g = lax.dot_general(ds, q, nn, preferred_element_type=f32)
        dv_g = lax.dot_general(p_b, do, nn, preferred_element_type=f32)
        if g == 0:
            dkv_ref[0, 0], dkv_ref[1, 0] = dk_g, dv_g
        else:
            dkv_ref[0, 0] += dk_g
            dkv_ref[1, 0] += dv_g


def attention(q_proj, do, kv, prefix_len, base, cos_tab, sin_tab, scale):
    batch, tokens, width = q_proj.shape
    e = kv.shape[2] // 2
    n_keys = kv.shape[1]
    heads = width // e
    cos_one = jnp.concatenate([cos_tab, cos_tab], axis=1)
    sin_one = jnp.concatenate([-sin_tab, sin_tab], axis=1)
    cos_full = jnp.tile(cos_one, (GROUP_HEADS, 1))
    sin_full = jnp.tile(sin_one, (GROUP_HEADS, 1))
    rows = GROUP_HEADS * tokens
    tok_spec = pl.BlockSpec((1, tokens, width), lambda b, *_: (b, 0, 0))
    kv_spec = pl.BlockSpec((1, n_keys, 2 * e), lambda b, *_: (b, 0, 0))
    dkv_spec = pl.BlockSpec((2, 1, n_keys, e), lambda b, *_: (0, b, 0, 0))
    tab_spec = pl.BlockSpec((rows, e), lambda b, *_: (0, 0))
    tab_t_spec = pl.BlockSpec((e, rows), lambda b, *_: (0, 0))
    flops = 6 * 2 * batch * heads * tokens * n_keys * e
    return pl.pallas_call(
        functools.partial(attention_kernel, heads, scale),
        grid_spec=pltpu.PrefetchScalarGridSpec(
            num_scalar_prefetch=2,
            grid=(batch,),
            in_specs=[tok_spec, tok_spec, kv_spec, tab_spec, tab_spec, tab_t_spec, tab_t_spec],
            out_specs=[tok_spec, tok_spec, dkv_spec],
            scratch_shapes=[pltpu.VMEM((n_keys, rows), jnp.float32)],
        ),
        out_shape=[
            jax.ShapeDtypeStruct((batch, tokens, width), jnp.bfloat16),
            jax.ShapeDtypeStruct((batch, tokens, width), jnp.bfloat16),
            jax.ShapeDtypeStruct((2, batch, n_keys, e), jnp.float32),
        ],
        cost_estimate=pl.CostEstimate(flops=2 * flops, bytes_accessed=q_proj.size * 10 + kv.size * 10, transcendentals=batch * heads * tokens * n_keys),
        compiler_params=pltpu.CompilerParams(dimension_semantics=("arbitrary",), vmem_limit_bytes=40 * 1024 * 1024),
        name="attention",
    )(prefix_len, base, q_proj, do, kv, cos_full, sin_full, cos_full.T, sin_full.T)


def norm_kernel(x_ref, gain_ref, normed_ref, normed_t_ref, inv_rms_ref):
    x = x_ref[...].astype(jnp.float32)
    inv_rms = lax.rsqrt(jnp.mean(x * x, axis=-1, keepdims=True) + NORM_EPS)
    normed = x * inv_rms * gain_ref[...]
    normed_ref[...] = normed.astype(jnp.bfloat16)
    normed_t_ref[...] = normed.T.astype(jnp.bfloat16)
    inv_rms_ref[...] = jnp.broadcast_to(inv_rms, inv_rms_ref.shape)


def norm_both_ways(x, gain):
    tokens, d_model = x.shape
    rows = 128
    return pl.pallas_call(
        norm_kernel,
        grid=(tokens // rows,),
        in_specs=[pl.BlockSpec((rows, d_model), lambda i: (i, 0)), pl.BlockSpec((1, d_model), lambda i: (0, 0))],
        out_specs=[pl.BlockSpec((rows, d_model), lambda i: (i, 0)), pl.BlockSpec((d_model, rows), lambda i: (0, i)), pl.BlockSpec((rows, 128), lambda i: (i, 0))],
        out_shape=[jax.ShapeDtypeStruct((tokens, d_model), jnp.bfloat16), jax.ShapeDtypeStruct((d_model, tokens), jnp.bfloat16), jax.ShapeDtypeStruct((tokens, 128), jnp.float32)],
        cost_estimate=pl.CostEstimate(flops=x.size * 20, bytes_accessed=x.size * 6, transcendentals=tokens),
        compiler_params=pltpu.CompilerParams(dimension_semantics=("arbitrary",), vmem_limit_bytes=32 * 1024 * 1024),
        name="norm",
    )(x, gain)


def wrap(j, n):
    return lax.rem(j + SHIFT, n)


def kv_shape(r, level):
    fixed = [(r + k) % 3 for k in range(level)]
    return tuple(1 if d in fixed else 2 for d in (2, 1, 0))


def weight_grad_kernel(plan, o_ref, dq_ref, dy_ref, xnt_ref, dyx0, dyx1, dyx2, xnx0, xnx1, xnx2, dkv_ref, x_ref, wo_ref, wq_ref, wkv_ref,
                       inv_rms_ref, gain_ref, cos_ref, sin_ref,
                       out_ref, y_ref, dxn_ref, dkvp_ref, rowdot_ref, dgain_ref,
                       b_buf, a_buf, part, core_land, acc4, land2, acc2, land3, gath, sib_land,
                       kv_own, kv_land0, kv_land1a, kv_land1b, kv_land1c, kv_land2a, kv_land2b, kv_land2c, kv_land3, gain_land,
                       job_a, job_wo, job_wq, job_wkv, job_x, job_acc, job_out,
                       send_sem, recv_sem, own_sem, sib_sem, a_sem, b_sem, kv_sem, gain_sem, job_sem, job_io_sem):
    units, first_q, base_o, base_q = plan
    steps = 2 * units
    dyx, xnx = (dyx0, dyx1, dyx2), (xnx0, xnx1, xnx2)
    kv_land1, kv_land2 = (kv_land1a, kv_land1b, kv_land1c), (kv_land2a, kv_land2b, kv_land2c)
    tokens, d_model = dy_ref.shape
    half = d_model // 2
    kv_pairs = dkv_ref.shape[0]
    seqs = kv_pairs // 2
    seq_tokens = dkv_ref.shape[5]
    jobs = d_model // JOB_COLS
    chunks = d_model // JOB_DEPTH
    me = lax.axis_index('sp')
    core = lax.rem(me, 2)
    sibling = me + 1 - 2 * core
    bits = [lax.rem(me // s, 2) for s in (2, 4, 8)]
    peers = [me + s * (1 - 2 * b) for s, b in zip((2, 4, 8), bits)]

    barrier = pltpu.get_barrier_semaphore()
    for peer in (sibling, *peers):
        pl.semaphore_signal(barrier, inc=1, device_id=(peer,), device_id_type=MESH_ID)
    pl.semaphore_wait(barrier, 4)

    def dims(r):
        d2, d3 = (r + 1) % 3, (r + 2) % 3
        return bits[r], bits[d2], bits[d3], peers[r], peers[d2], peers[d3]

    def remote(r, stage, j, src, dst, peer):
        slot = wrap(j, 2)
        return pltpu.make_async_remote_copy(src_ref=src, dst_ref=dst, send_sem=send_sem.at[r, stage, slot], recv_sem=recv_sem.at[r, stage, slot],
                                            device_id=(peer,), device_id_type=MESH_ID)

    def kv_pick(r, level, flip):
        picks = {}
        for k in range(3):
            d = (r + k) % 3
            picks[d] = pl.ds(bits[d], 1) if k < level else pl.ds(0, 2)
        if flip:
            d = (r + level) % 3
            picks[d] = pl.ds(1 - bits[d], 1)
        return picks[2], picks[1], picks[0]

    def transfer(r, stage, j):
        b1, b2, b3, p1, p2, p3 = dims(r)
        two = wrap(j, 2)
        g = wrap(j, AG_DEPTH)
        if stage == ST_CORE:
            return remote(r, stage, j, part.at[r, two, pl.ds((1 - core) * 4, 4)], core_land.at[r, two], sibling)
        if stage == ST_RS2:
            return remote(r, stage, j, acc4.at[r, two, pl.ds((1 - b2) * 2, 2)], land2.at[r, two], p2)
        if stage == ST_RS3:
            return remote(r, stage, j, acc2.at[r, two, pl.ds(1 - b3, 1)], land3.at[r, two], p3)
        if stage == ST_AG3:
            ref = gath.at[r, g, pl.ds(b1 * 4 + b2 * 2 + b3, 1)]
            return remote(r, stage, j, ref, ref, p3)
        if stage == ST_AG2:
            ref = gath.at[r, g, pl.ds(b1 * 4 + b2 * 2, 2)]
            return remote(r, stage, j, ref, ref, p2)
        if stage == ST_AG1:
            ref = gath.at[r, g, pl.ds(b1 * 4, 4)]
            return remote(r, stage, j, ref, ref, p1)
        if stage == ST_SIB:
            return remote(r, stage, j, gath.at[r, g], sib_land.at[r, wrap(j, SIB_DEPTH)], sibling)
        if stage == ST_A:
            a = wrap(j, A_DEPTH)
            return remote(r, stage, j, a_buf.at[r, a, pl.ds(0, tokens)], a_buf.at[r, a, pl.ds(tokens, tokens)], p1)
        if stage == ST_K0:
            return remote(r, stage, j, dkv_ref.at[3 * j + r, :, :, :, 1 - core], kv_land0.at[r, two], sibling)
        level = stage - ST_K1
        src = kv_own.at[(r, wrap(j, KV_DEPTH), *kv_pick(r, level, True))]
        land = kv_land3.at[r, two] if level == 2 else (kv_land1, kv_land2)[level][r].at[two]
        return remote(r, stage, j, src, land, (p1, p2, p3)[level])

    def is_q(r, unit):
        return jnp.where(unit >= first_q[r], 1, 0)

    def writes(r, j, whose, src, sem):
        unit = (j + SHIFT) // 2 - SHIFT // 2
        q = wrap(j, 2)
        m = is_q(r, unit)
        head = (base_o[r] + unit) * (1 - m) + (base_q[r] + unit - first_q[r]) * m
        copies = []
        for idx in range(SUB_TILES):
            tile = (idx // 4) * 16 + q * 8 + whose * 4 + idx % 4
            row = pl.multiple_of((head * (1 - m) + tile * m) * TILE, TILE)
            col = pl.multiple_of((tile * (1 - m) + head * m) * TILE, TILE)
            copies.append(pltpu.make_async_copy(src.at[idx], out_ref.at[m, pl.ds(row, TILE), pl.ds(col, TILE)], sem.at[r, idx]))
        return copies

    def own_writes(r, j):
        return writes(r, j, core, gath.at[r, wrap(j, AG_DEPTH)], own_sem)

    def sib_writes(r, j):
        return writes(r, j, 1 - core, sib_land.at[r, wrap(j, SIB_DEPTH)], sib_sem)

    def a_load(r, unit, source):
        head = base_q[r] + unit - first_q[r] if source is dq_ref else base_o[r] + unit
        col = pl.multiple_of(head * TILE, TILE)
        return pltpu.make_async_copy(source.at[:, pl.ds(col, TILE)], a_buf.at[r, wrap(unit, A_DEPTH), pl.ds(0, tokens)], a_sem.at[r])

    def b_load(r, q_phase):
        start = pl.multiple_of(bits[r] * half, half)
        if q_phase:
            return [pltpu.make_async_copy(xnt_ref.at[pl.ds(start, half), :], b_buf.at[r, :, pl.ds(0, tokens)], b_sem.at[r, 0]),
                    pltpu.make_async_copy(xnx[r], b_buf.at[r, :, pl.ds(tokens, tokens)], b_sem.at[r, 1])]
        return [pltpu.make_async_copy(dy_ref.at[:, pl.ds(start, half)], b_buf.at[r, pl.ds(0, tokens), :], b_sem.at[r, 0]),
                pltpu.make_async_copy(dyx[r], b_buf.at[r, pl.ds(tokens, tokens), :], b_sem.at[r, 1])]

    def kv_load(r, j):
        return pltpu.make_async_copy(dkv_ref.at[3 * j + r, :, :, :, core], kv_own.at[r, wrap(j, KV_DEPTH)], kv_sem.at[r])

    def valid(j, n):
        return (j >= 0) & (j < n)

    def job_cols(n):
        return pl.ds(pl.multiple_of(n * JOB_COLS, JOB_COLS), JOB_COLS)

    def job_loads(back, n, kc):
        depth = pl.ds(pl.multiple_of(kc * JOB_DEPTH, JOB_DEPTH), JOB_DEPTH)
        two = lax.rem(kc, 2)
        if back:
            return [pltpu.make_async_copy(dq_ref.at[:, depth], job_a.at[two], job_sem.at[two, 0]),
                    pltpu.make_async_copy(wq_ref.at[job_cols(n), depth], job_wq.at[two], job_sem.at[two, 1])]
        return [pltpu.make_async_copy(o_ref.at[:, depth], job_a.at[two], job_sem.at[two, 0]),
                pltpu.make_async_copy(wo_ref.at[depth, job_cols(n)], job_wo.at[two], job_sem.at[two, 1])]

    def job_x_load(n):
        return pltpu.make_async_copy(x_ref.at[:, job_cols(n)], job_x, job_io_sem.at[0])

    def job_wkv_load(n):
        return pltpu.make_async_copy(wkv_ref.at[job_cols(n), :], job_wkv, job_io_sem.at[1])

    def job_store(back, n):
        return pltpu.make_async_copy(job_out, (dxn_ref if back else y_ref).at[:, job_cols(n)], job_io_sem.at[2])

    def job_begin(t):
        for back in (False, True):
            n = t - JOB_FIRST - (jobs if back else 0)

            @pl.when(valid(n, jobs))
            def _(back=back, n=n):
                for copy in job_loads(back, n, 0):
                    copy.start()
                job_x_load(n).start()
                if back:
                    job_wkv_load(n).start()
                job_acc[...] = jnp.zeros_like(job_acc)

    def job_part(t, lo, hi):
        for back in (False, True):
            n = t - JOB_FIRST - (jobs if back else 0)

            @pl.when(valid(n, jobs))
            def _(back=back, n=n):
                def chunk(kc, carry):
                    @pl.when(kc + 1 < chunks)
                    def _():
                        for copy in job_loads(back, n, kc + 1):
                            copy.start()
                    for copy in job_loads(back, n, kc):
                        copy.wait()
                    two = lax.rem(kc, 2)
                    if back:
                        job_acc[...] += lax.dot_general(job_a[two], job_wq[two], NT, preferred_element_type=jnp.float32)
                    else:
                        job_acc[...] += jnp.dot(job_a[two], job_wo[two], preferred_element_type=jnp.float32)
                    return carry
                lax.fori_loop(lo, hi, chunk, 0)

    def job_end(t):
        for back in (False, True):
            n = t - JOB_FIRST - (jobs if back else 0)

            @pl.when(valid(n, jobs))
            def _(back=back, n=n):
                job_x_load(n).wait()

                if back:
                    job_wkv_load(n).wait()
                    job_store(False, 0).wait()
                    job_acc[...] += lax.dot_general(dkvp_ref[...], job_wkv[...], NT, preferred_element_type=jnp.float32)
                    for h in range(JOB_COLS // TILE):
                        cols = slice(h * TILE, (h + 1) * TILE)
                        grad = job_acc[:, cols].astype(jnp.bfloat16)
                        job_out[:, cols] = grad
                        grad = grad.astype(jnp.float32)
                        x_cols = job_x[:, cols].astype(jnp.float32)
                        scaled = grad * gain_ref[:, pl.ds(pl.multiple_of(n * JOB_COLS + h * TILE, TILE), TILE)] * x_cols

                        @pl.when(n + h == 0)
                        def _():
                            rowdot_ref[...] = scaled

                        @pl.when(n + h > 0)
                        def _():
                            rowdot_ref[...] += scaled
                        dgain_ref[n * 2 + h] = jnp.sum((grad * x_cols * inv_rms_ref[...]).reshape(tokens // 8, 8, TILE), axis=0)
                else:
                    @pl.when(n > 0)
                    def _():
                        job_store(False, 0).wait()
                    job_out[...] = (job_x[...].astype(jnp.float32) + job_acc[...]).astype(jnp.bfloat16)
                job_store(back, n).start()

    gain_peers = (sibling, *peers)

    def gain_send(k):
        return pltpu.make_async_remote_copy(src_ref=dgain_ref, dst_ref=gain_land.at[k], send_sem=gain_sem.at[k, 0], recv_sem=gain_sem.at[k, 1],
                                            device_id=(gain_peers[k],), device_id_type=MESH_ID)

    lags = {ST_CORE: 0, ST_RS2: 1, ST_RS3: 2, ST_AG3: 3, ST_AG2: 4, ST_AG1: 5, ST_SIB: 6}
    kv_lags = {ST_K0: 0, ST_K1: 1, ST_K2: 2, ST_K3: 3}
    job_split = (0, chunks * 3 // 8, chunks * 6 // 8, chunks)

    for r in range(ROTATIONS):
        for copy in b_load(r, False):
            copy.start()

    def slot(i, carry):
        t = i - 3
        odd = lax.rem(i + 1, 2) == 1
        job_begin(t)
        for k in range(len(gain_peers) + 1):
            @pl.when(t == GAIN_FIRST + k)
            def _(k=k):
                if k > 0:
                    copy = gain_send(k - 1)
                    copy.wait_recv()
                    copy.wait_send()
                    dgain_ref[...] += gain_land[k - 1]
                if k < len(gain_peers):
                    gain_send(k).start()

        for r in range(ROTATIONS):
            b1, b2, b3, _, _, _ = dims(r)
            kv_items = (kv_pairs - r + 2) // 3
            for stage, lag in (lags | kv_lags).items():
                j = t - 1 - lag

                @pl.when(valid(j, kv_items if stage >= ST_K0 else steps))
                def _(stage=stage, j=j):
                    copy = transfer(r, stage, j)
                    copy.wait_recv()
                    copy.wait_send()

            @pl.when(valid(t - 7, steps))
            def _():
                for copy in own_writes(r, t - 7):
                    copy.wait()

            @pl.when(valid(t - 8, steps))
            def _():
                for copy in sib_writes(r, t - 8):
                    copy.wait()

            @pl.when(valid(t - 1, steps))
            def _():
                two = wrap(t - 1, 2)
                acc4[r, two] = part[r, two, pl.ds(core * 4, 4)] + core_land[r, two]

            @pl.when(valid(t - 2, steps))
            def _():
                two = wrap(t - 2, 2)
                acc2[r, two] = acc4[r, two, pl.ds(b2 * 2, 2)] + land2[r, two]

            @pl.when(valid(t - 3, steps))
            def _():
                two = wrap(t - 3, 2)
                gath[r, wrap(t - 3, AG_DEPTH), pl.ds(b1 * 4 + b2 * 2 + b3, 1)] = acc2[r, two, pl.ds(b3, 1)] + land3[r, two]

            @pl.when(valid(t - 1, kv_items))
            def _():
                kv_load(r, t - 1).wait()
                d = wrap(t - 1, KV_DEPTH)
                kv_own[r, d] += kv_land0[r, wrap(t - 1, 2)]

            @pl.when(valid(t - 2, kv_items))
            def _():
                mine = (r, wrap(t - 2, KV_DEPTH), *kv_pick(r, 1, False))
                kv_own[mine] += kv_land1[r][wrap(t - 2, 2)]

            @pl.when(valid(t - 3, kv_items))
            def _():
                mine = (r, wrap(t - 3, KV_DEPTH), *kv_pick(r, 2, False))
                kv_own[mine] += kv_land2[r][wrap(t - 3, 2)]

            @pl.when(valid(t - 4, kv_items))
            def _():
                pair = 3 * (t - 4) + r
                kv = pair // seqs
                mine = (r, wrap(t - 4, KV_DEPTH), *kv_pick(r, 3, False))
                total = (kv_own[mine] + kv_land3[r, wrap(t - 4, 2)]).reshape(seq_tokens, TILE)
                total = total.astype(jnp.bfloat16).astype(jnp.float32)
                total = total * cos_ref[kv] - pltpu.roll(total, TILE // 2, 1) * sin_ref[kv]
                row = pl.multiple_of((pair - kv * seqs) * seq_tokens, seq_tokens)
                dkvp_ref[pl.ds(row, seq_tokens), pl.ds(pl.multiple_of(kv * TILE, TILE), TILE)] = total.astype(jnp.bfloat16)

            for stage, lag in (lags | kv_lags).items():
                j = t - lag

                @pl.when(valid(j, kv_items if stage >= ST_K0 else steps))
                def _(stage=stage, j=j):
                    transfer(r, stage, j).start()

            @pl.when(valid(t, kv_items))
            def _():
                kv_load(r, t).start()

            @pl.when(valid(t - 6, steps))
            def _():
                for copy in own_writes(r, t - 6):
                    copy.start()

            @pl.when(valid(t - 7, steps))
            def _():
                for copy in sib_writes(r, t - 7):
                    copy.start()

            nxt = (t + 3) // 2
            for source, lo, hi in ((o_ref, 0, first_q[r]), (dq_ref, first_q[r], units)):
                @pl.when(odd & (nxt >= lo) & (nxt < hi))
                def _(source=source):
                    a_load(r, nxt, source).start()

                @pl.when(jnp.logical_not(odd) & ((t + 2) // 2 >= lo) & ((t + 2) // 2 < hi))
                def _(source=source):
                    a_load(r, (t + 2) // 2, source).wait()
                    transfer(r, ST_A, (t + 2) // 2).start()

            @pl.when(odd & valid((t + 1) // 2, units))
            def _():
                copy = transfer(r, ST_A, (t + 1) // 2)
                copy.wait_recv()
                copy.wait_send()

            j = t + 1
            q = wrap(j, 2)
            two = wrap(j, 2)
            unit = (j + SHIFT) // 2 - SHIFT // 2
            a_slot = wrap(unit, A_DEPTH)

            @pl.when(j == 0)
            def _():
                for copy in b_load(r, False):
                    copy.wait()

            @pl.when(j == 2 * first_q[r])
            def _():
                copies = b_load(r, True)
                for copy in copies:
                    copy.start()
                for copy in copies:
                    copy.wait()

            @pl.when((j >= 0) & (j < 2 * first_q[r]))
            def _():
                a_t = a_buf[r, a_slot].T
                for n in range(4):
                    res = jnp.dot(a_t, b_buf[r, :, pl.ds(pl.multiple_of(q * 1024 + n * 256, 256), 256)], preferred_element_type=jnp.float32)
                    part[r, two, 2 * n] = res[:, :TILE]
                    part[r, two, 2 * n + 1] = res[:, TILE:]

            @pl.when((j >= 2 * first_q[r]) & (j < steps))
            def _():
                a = a_buf[r, a_slot]
                for n in range(4):
                    res = jnp.dot(b_buf[r, pl.ds(pl.multiple_of(q * 1024 + n * 256, 256), 256), :], a, preferred_element_type=jnp.float32)
                    part[r, two, 2 * n] = res[:TILE]
                    part[r, two, 2 * n + 1] = res[TILE:]

            job_part(t, job_split[r], job_split[r + 1])
        job_end(t)
        return carry

    last = max(steps + 8, GAIN_FIRST + len(gain_peers) + 1)
    lax.fori_loop(0, last + 3, slot, 0)
    job_store(True, 0).wait()


def weight_grads(o, dq, dy, xnt, dyx, xnx, dkv_part, x, w_o, w_q, w_kv, inv_rms, gain, cos_kv, sin_kv, plan):
    tokens, width = o.shape
    d_model = dy.shape[1]
    f32, bf16 = jnp.float32, jnp.bfloat16
    any_spec = pl.BlockSpec(memory_space=pl.ANY)
    vmem_spec = pl.BlockSpec(memory_space=pltpu.VMEM)
    tile = (TILE, TILE)
    units = plan[0]
    pairs, seq_keys = dkv_part.shape[0] * dkv_part.shape[1], dkv_part.shape[2]
    piece = (seq_keys // 16, TILE)
    dkv_part = dkv_part.reshape(pairs, 2, 2, 2, 2, *piece)
    return pl.pallas_call(
        functools.partial(weight_grad_kernel, plan),
        in_specs=[any_spec] * 15 + [vmem_spec] * 4,
        out_specs=[any_spec] * 3 + [vmem_spec] * 3,
        out_shape=[
            jax.ShapeDtypeStruct((2, width, d_model), f32),
            jax.ShapeDtypeStruct((tokens, d_model), bf16),
            jax.ShapeDtypeStruct((tokens, d_model), bf16),
            jax.ShapeDtypeStruct((tokens, 2 * TILE), bf16),
            jax.ShapeDtypeStruct((tokens, TILE), f32),
            jax.ShapeDtypeStruct((d_model // TILE, 8, TILE), f32),
        ],
        scratch_shapes=[
            pltpu.VMEM((ROTATIONS, 2 * tokens, d_model // 2), bf16),
            pltpu.VMEM((ROTATIONS, A_DEPTH, 2 * tokens, TILE), bf16),
            pltpu.VMEM((ROTATIONS, 2, 8, *tile), f32),
            pltpu.VMEM((ROTATIONS, 2, 4, *tile), f32),
            pltpu.VMEM((ROTATIONS, 2, 4, *tile), f32),
            pltpu.VMEM((ROTATIONS, 2, 2, *tile), f32),
            pltpu.VMEM((ROTATIONS, 2, 2, *tile), f32),
            pltpu.VMEM((ROTATIONS, 2, 1, *tile), f32),
            pltpu.VMEM((ROTATIONS, AG_DEPTH, 8, *tile), f32),
            pltpu.VMEM((ROTATIONS, SIB_DEPTH, 8, *tile), f32),
            pltpu.VMEM((ROTATIONS, KV_DEPTH, 2, 2, 2, *piece), f32),
            pltpu.VMEM((ROTATIONS, 2, 2, 2, 2, *piece), f32),
            *[pltpu.VMEM((2, *kv_shape(r, 1), *piece), f32) for r in range(ROTATIONS)],
            *[pltpu.VMEM((2, *kv_shape(r, 2), *piece), f32) for r in range(ROTATIONS)],
            pltpu.VMEM((ROTATIONS, 2, 1, 1, 1, *piece), f32),
            pltpu.VMEM((4, d_model // TILE, 8, TILE), f32),
            pltpu.VMEM((2, tokens, JOB_DEPTH), bf16),
            pltpu.VMEM((2, JOB_DEPTH, JOB_COLS), bf16),
            pltpu.VMEM((2, JOB_COLS, JOB_DEPTH), bf16),
            pltpu.VMEM((JOB_COLS, 2 * TILE), bf16),
            pltpu.VMEM((tokens, JOB_COLS), bf16),
            pltpu.VMEM((tokens, JOB_COLS), f32),
            pltpu.VMEM((tokens, JOB_COLS), bf16),
            pltpu.SemaphoreType.DMA((ROTATIONS, STAGES, 2)),
            pltpu.SemaphoreType.DMA((ROTATIONS, STAGES, 2)),
            pltpu.SemaphoreType.DMA((ROTATIONS, SUB_TILES)),
            pltpu.SemaphoreType.DMA((ROTATIONS, SUB_TILES)),
            pltpu.SemaphoreType.DMA((ROTATIONS,)),
            pltpu.SemaphoreType.DMA((ROTATIONS, 2)),
            pltpu.SemaphoreType.DMA((ROTATIONS,)),
            pltpu.SemaphoreType.DMA((4, 2)),
            pltpu.SemaphoreType.DMA((2, 2)),
            pltpu.SemaphoreType.DMA((3,)),
        ],
        cost_estimate=pl.CostEstimate(flops=ROTATIONS * units * 2 * TILE * d_model * tokens * 2, bytes_accessed=800 * 1024 * 1024, transcendentals=0),
        compiler_params=pltpu.CompilerParams(collective_id=0, has_side_effects=True, vmem_limit_bytes=67043328),
        name="weight_grads",
    )(o, dq, dy, xnt, *dyx, *xnx, dkv_part, x, w_o, w_q, w_kv, inv_rms, gain, cos_kv, sin_kv)


def unit_plan(heads_o, heads_q):
    units = (heads_o + heads_q) // ROTATIONS
    share_o = [heads_o // ROTATIONS + (1 if r < heads_o % ROTATIONS else 0) for r in range(ROTATIONS)]
    base_o = [sum(share_o[:r]) for r in range(ROTATIONS)]
    share_q = [units - s for s in share_o]
    base_q = [sum(share_q[:r]) for r in range(ROTATIONS)]
    return units, tuple(share_o), tuple(base_o), tuple(base_q)


def solution(mesh):
    groups = mesh.shape['sp']
    seq_spec = P(None, 'sp', None)
    whole = P()

    def local_block(x, dy, prefix_len, w_norm, w_q, w_k, w_v, w_o):
        batch, tokens, d_model = x.shape
        head_dim = w_k.shape[1]
        heads = w_q.shape[1] // head_dim
        scale = head_dim ** -0.5
        my_index = lax.axis_index('sp')
        f32 = jnp.float32
        flat = batch * tokens
        half = d_model // 2

        x2 = x.reshape(flat, d_model)
        dy2 = dy.reshape(flat, d_model)
        gain = (1.0 + w_norm.astype(f32)).reshape(1, d_model)
        normed, normed_t, inv_rms = norm_both_ways(x2, gain)
        dyx, xnx = [], []
        for stride in (2, 4, 8):
            pairs = [(i, i ^ stride) for i in range(groups)]
            start = (1 - (my_index // stride) % 2) * half
            dyx.append(lax.ppermute(lax.dynamic_slice(dy2, (0, start), (flat, half)), 'sp', pairs))
            xnx.append(lax.ppermute(lax.dynamic_slice(normed_t, (start, 0), (half, flat)), 'sp', pairs))

        base = my_index * tokens
        cos_tab, sin_tab = rope_tables(base + jnp.arange(tokens), head_dim)
        cos_kv = jnp.stack([jnp.concatenate([cos_tab, cos_tab], axis=1), jnp.ones((tokens, head_dim), f32)])
        sin_kv = jnp.stack([jnp.concatenate([-sin_tab, sin_tab], axis=1), jnp.zeros((tokens, head_dim), f32)])
        normed3 = normed.reshape(batch, tokens, d_model)
        w_kv = jnp.concatenate([w_k, w_v], axis=1)
        kv_own = jnp.einsum('bsd,de->bse', normed3, w_kv, preferred_element_type=f32)
        k_own = apply_rope(kv_own[..., :head_dim], cos_tab, sin_tab).astype(jnp.bfloat16)
        v_own = kv_own[..., head_dim:].astype(jnp.bfloat16)
        kv = lax.all_gather(jnp.concatenate([k_own, v_own], axis=-1), 'sp', axis=1, tiled=True)
        q_proj = jnp.einsum('bsd,de->bse', normed3, w_q, preferred_element_type=f32)
        do = jnp.einsum('bsd,ed->bse', dy, w_o, preferred_element_type=f32).astype(jnp.bfloat16)
        o, dq_proj, dkv_part = attention(q_proj, do, kv, prefix_len, base.reshape(1), cos_tab, sin_tab, scale)

        dq2 = dq_proj.reshape(flat, d_model)
        summed, y_out, d_normed, dkv_proj, row_dot, d_gain = weight_grads(
            o.reshape(flat, d_model), dq2, dy2, normed_t, dyx, xnx, dkv_part, x2, w_o, w_q, w_kv, inv_rms, gain, cos_kv, sin_kv,
            unit_plan(heads, KERNEL_Q_HEADS))

        rest = KERNEL_Q_HEADS * head_dim
        d_rest = lax.psum(jnp.dot(normed_t, jnp.concatenate([dq2[:, rest:], dkv_proj], axis=1), preferred_element_type=f32), 'sp')
        inv = inv_rms[:, :1]
        mean_dot = jnp.sum(row_dot, axis=1, keepdims=True) / d_model
        dx_norm = d_normed.astype(f32) * gain * inv - x2.astype(f32) * (mean_dot * inv * inv * inv)
        dx_out = (dy2.astype(f32) + dx_norm).astype(jnp.bfloat16)
        d_wo = summed[0]
        left = d_model - rest
        d_wq = lax.dynamic_update_slice(summed[1], d_rest[:, :left], (0, rest))
        d_wk = d_rest[:, left:left + head_dim]
        d_wv = d_rest[:, left + head_dim:]
        return (y_out.reshape(batch, tokens, d_model), dx_out.reshape(batch, tokens, d_model), d_wq, d_wk, d_wv, d_wo,
                jnp.sum(d_gain, axis=1).reshape(d_model))

    return jax.shard_map(local_block, mesh=mesh, in_specs=(seq_spec, seq_spec, whole, whole, whole, whole, whole, whole), out_specs=(seq_spec, seq_spec, whole, whole, whole, whole, whole), check_vma=False)
```
